32 devices in a mesh: far: 4 (over z), near: 8 (over y, x, core).
Axes of the slice: x: 2, y: 2, z: 4, core: 2. Of those that a mesh axis runs over, the one named last changes fastest.
Arguments:
- state_real: float32 [4, 8, 2, 128, 128], P('far', 'near'), may hold values from -5 to 5
- state_imag: float32 [4, 8, 2, 128, 128], P('far', 'near'), may hold values from -5 to 5
- gate_real: float32 [2, 4, 3, 128, 128], replicated, may hold values from -0.375 to 0.375
- gate_imag: float32 [2, 4, 3, 128, 128], replicated, may hold values from -0.375 to 0.375
Outputs:
- final_real: float32 [4, 8, 2, 128, 128], P('far', 'near')
- final_imag: float32 [4, 8, 2, 128, 128], P('far', 'near')
The draws below stay inside these ranges and needn't reach their ends.
All inputs are finite; a program needn't handle non-finite values.
Results may differ from the reference program's by a relative error of at most 0.000071.
Values sent between devices are 32-bit elements; how exact they have to be, the bound alone decides.
A program may use at most 64 MiB of HBM per device.

```python
import jax
import jax.numpy as jnp
from jax import lax

GATE = 128
HIGH = 2
ROUNDS = 2
SECTIONS = 4
DEPTH = 3
N_FAR = 4
N_NEAR = 8


def shard_levels(key, shape, cuts, low, high):
    level = 1.0
    for axis_at, parts in cuts:
        heights = jax.random.uniform(jax.random.fold_in(jax.random.fold_in(key, 6), axis_at), (parts,), jnp.float32, low / len(cuts), high / len(cuts))
        level = level * jnp.repeat(jnp.exp(heights), shape[axis_at] // parts).reshape((-1,) + (1,) * (len(shape) - 1 - axis_at))
    return level


def noise(rng, dims, spread, most, cuts=(), kind=jnp.bfloat16):
    array = spread * jax.random.normal(rng, dims, jnp.float32)
    if cuts:
        array = array * shard_levels(rng, dims, cuts, -0.22, 0.18)
    return jnp.clip(array, -most, most).astype(kind)


def setup_inputs(seed: int = 0) -> dict:
    arg_keys = jax.random.split(jax.random.key(seed), 5)
    return {
        "state_real": noise(arg_keys[0], (N_FAR, N_NEAR, HIGH, GATE, GATE), 0.7, 5.0, ((0, 4), (1, 8)), jnp.float32),
        "state_imag": noise(arg_keys[1], (N_FAR, N_NEAR, HIGH, GATE, GATE), 0.7, 5.0, ((0, 4), (1, 8)), jnp.float32),
        "gate_real": noise(arg_keys[2], (ROUNDS, SECTIONS, DEPTH, GATE, GATE), (2 * GATE) ** -0.5, 0.375, (), jnp.float32),
        "gate_imag": noise(arg_keys[3], (ROUNDS, SECTIONS, DEPTH, GATE, GATE), (2 * GATE) ** -0.5, 0.375, (), jnp.float32),
    }


def gate_low(x, g):
    return jnp.einsum('...l,jl->...j', x, g, precision=lax.Precision.HIGHEST, preferred_element_type=jnp.float32)


def gate_mid(x, g):
    return jnp.einsum('...ml,jm->...jl', x, g, precision=lax.Precision.HIGHEST, preferred_element_type=jnp.float32)


def gate_top(x, g):
    high, width, lows = x.shape[-3], x.shape[-2], x.shape[-1]
    upper = g.shape[0] // high
    lead = x.shape[:-3]
    viewed = x.reshape(lead + (high, upper, width // upper, lows))
    matrix = g.reshape((g.shape[0], high, upper))
    out = jnp.einsum('...hkrl,jhk->...jrl', viewed, matrix, precision=lax.Precision.HIGHEST, preferred_element_type=jnp.float32)
    return out.reshape(lead + (high, width, lows))


def complex_gate(form, real, imag, greal, gimag):
    new_real = form(real, greal) - form(imag, gimag)
    new_imag = form(imag, greal) + form(real, gimag)
    return new_real, new_imag


def swap_far(x):
    nfar, nnear, high, width, lows = x.shape
    y = x.reshape((nfar, nnear, nfar, high * width // nfar, lows))
    return jnp.swapaxes(y, 0, 2).reshape(x.shape)


def swap_mid(x):
    nfar, nnear, high, width, lows = x.shape
    y = x.reshape((nfar, nnear, high, nnear, width // nnear, lows))
    return jnp.swapaxes(y, 1, 3).reshape(x.shape)


def swap_low(x):
    nfar, nnear, high, width, lows = x.shape
    y = x.reshape((nfar, nnear, high, width, nnear, lows // nnear))
    return jnp.swapaxes(y, 1, 4).reshape(x.shape)


def swap_top(x):
    nfar, nnear, high, width, lows = x.shape
    y = x.reshape((nfar, nnear, nnear, high * width // nnear, lows))
    return jnp.swapaxes(y, 1, 2).reshape(x.shape)


def reference(state_real, state_imag, gate_real, gate_imag):
    real, imag = state_real, state_imag
    swaps = (swap_far, swap_mid, swap_low, swap_top)
    forms = (gate_low, gate_mid, gate_top)
    for rnd in range(ROUNDS):
        for section in range(4):
            real = swaps[section](real)
            imag = swaps[section](imag)
            for which in range(3):
                real, imag = complex_gate(forms[which], real, imag, gate_real[rnd, section, which], gate_imag[rnd, section, which])
    return real, imag
```

```python
import functools

import jax
import jax.numpy as jnp
from jax import lax
from jax.experimental import pallas as pl
from jax.experimental.pallas import tpu as pltpu
from jax.sharding import PartitionSpec as P


def gate_low(x, g):
    return jnp.einsum(
        "...l,jl->...j", x, g, precision=lax.Precision.HIGHEST, preferred_element_type=jnp.float32
    )


def gate_mid(x, g):
    return jnp.einsum(
        "...ml,jm->...jl", x, g, precision=lax.Precision.HIGHEST, preferred_element_type=jnp.float32
    )


def gate_top(x, g):
    high, width, lows = (x.shape[-3], x.shape[-2], x.shape[-1])
    upper = g.shape[0] // high
    lead = x.shape[:-3]
    viewed = x.reshape(lead + (high, upper, width // upper, lows))
    matrix = g.reshape((g.shape[0], high, upper))
    out = jnp.einsum(
        "...hkrl,jhk->...jrl",
        viewed,
        matrix,
        precision=lax.Precision.HIGHEST,
        preferred_element_type=jnp.float32,
    )
    return out.reshape(lead + (high, width, lows))


def complex_gate(form, real, imag, greal, gimag):
    new_real = form(real, greal) - form(imag, gimag)
    new_imag = form(imag, greal) + form(real, gimag)
    return (new_real, new_imag)


def merged_rows(x):
    return x.reshape((1, 1, x.shape[2] * x.shape[3], x.shape[4]))


def on_device(state_real, state_imag, gate_real, gate_imag):
    real, imag = (state_real, state_imag)
    forms = (gate_low, gate_mid, gate_top)
    shape = state_real.shape
    for rnd in range(gate_real.shape[0]):
        for section in range(4):
            if section == 2:
                order = [1, 0, 2]
            else:
                order = [0, 1, 2]
            early = []
            later = order[len(early) :]
            pair = (real, imag)
            if section == 0:
                moved = (
                    lax.all_to_all(
                        merged_rows(pair[0]), "far", split_axis=2, concat_axis=2, tiled=True
                    ),
                    lax.all_to_all(
                        merged_rows(pair[1]), "far", split_axis=2, concat_axis=2, tiled=True
                    ),
                )
                pair = (moved[0].reshape(shape), moved[1].reshape(shape))
            elif section == 1:
                pair = (
                    lax.all_to_all(pair[0], "near", split_axis=3, concat_axis=3, tiled=True),
                    lax.all_to_all(pair[1], "near", split_axis=3, concat_axis=3, tiled=True),
                )
            elif section == 2:
                pair = (
                    lax.all_to_all(pair[0], "near", split_axis=4, concat_axis=4, tiled=True),
                    lax.all_to_all(pair[1], "near", split_axis=4, concat_axis=4, tiled=True),
                )
            else:
                moved = (
                    lax.all_to_all(
                        merged_rows(pair[0]), "near", split_axis=2, concat_axis=2, tiled=True
                    ),
                    lax.all_to_all(
                        merged_rows(pair[1]), "near", split_axis=2, concat_axis=2, tiled=True
                    ),
                )
                pair = (moved[0].reshape(shape), moved[1].reshape(shape))
            for which in later:
                pair = complex_gate(
                    forms[which],
                    pair[0],
                    pair[1],
                    gate_real[rnd, section, which],
                    gate_imag[rnd, section, which],
                )
            real, imag = pair
    return (real, imag)


def dot(a, b, dims):
    return lax.dot_general(
        a, b, (dims, ((), ())), precision=lax.Precision.HIGHEST, preferred_element_type=jnp.float32
    )


def complex_matrix(greal, gimag):
    return jnp.concatenate(
        [jnp.concatenate([greal, -gimag], axis=1), jnp.concatenate([gimag, greal], axis=1)], axis=0
    )


def kernel(sizes, sr_ref, si_ref, gr_hbm, gi_hbm, or_ref, oi_ref, *scratch):
    nfar, nnear, rounds, high, order, lows = sizes
    sections = 4 * rounds
    sends, recvs = scratch[: sections - 1], scratch[sections - 1 : 2 * sections - 1]
    gr_ref, gi_ref, x_ref, send_sem, recv_sem, own_sem, gate_sem = scratch[2 * sections - 1 :]
    far, near = lax.axis_index("far"), lax.axis_index("near")
    upper = order // high
    rest = order // upper

    loads = [
        pltpu.make_async_copy(gr_hbm, gr_ref, gate_sem.at[0]),
        pltpu.make_async_copy(gi_hbm, gi_ref, gate_sem.at[1]),
    ]
    for load in loads:
        load.start()
    barrier = pltpu.get_barrier_semaphore()
    for k in range(1, nfar):
        pl.semaphore_signal(
            barrier, inc=1, device_id=(lax.rem(far + k, nfar), near), device_id_type=pl.DeviceIdType.MESH
        )
    for k in range(1, nnear):
        pl.semaphore_signal(
            barrier, inc=1, device_id=(far, lax.rem(near + k, nnear)), device_id_type=pl.DeviceIdType.MESH
        )
    pl.semaphore_wait(barrier, nfar - 1 + nnear - 1)

    pending = []

    def exchange(step):
        n, me = (nfar, far) if step % 4 == 0 else (nnear, near)
        recv = recvs[step]
        waits = []
        for k in range(1, n):
            to = lax.rem(me + k, n)
            for c in range(2):
                block = (sr_ref, si_ref)[c].at[to] if step == 0 else sends[step - 1].at[c, to]
                device = (to, near) if step % 4 == 0 else (far, to)
                copy = pltpu.make_async_remote_copy(
                    src_ref=block,
                    dst_ref=recv.at[c, me],
                    send_sem=send_sem.at[step, c, k],
                    recv_sem=recv_sem.at[step, c, k],
                    device_id=device,
                    device_id_type=pl.DeviceIdType.MESH,
                )
                copy.start()
                pending.append(copy)
                origin = lax.rem(me + n - k, n)
                waits.append(
                    pltpu.make_async_remote_copy(
                        src_ref=recv.at[c, origin],
                        dst_ref=recv.at[c, origin],
                        send_sem=send_sem.at[step, c, k],
                        recv_sem=recv_sem.at[step, c, k],
                        device_id=device,
                        device_id_type=pl.DeviceIdType.MESH,
                    )
                )
        for c in range(2):
            block = (sr_ref, si_ref)[c].at[me] if step == 0 else sends[step - 1].at[c, me]
            own = pltpu.make_async_copy(block, recv.at[c, me], own_sem.at[step, c])
            own.start()
            own.wait()
        if step == 0:
            for load in loads:
                load.wait()
        for wait in waits:
            wait.wait_recv()

    def tops(x):
        pieces = []
        for c in range(2):
            for h in range(high):
                pieces.append(
                    jnp.concatenate(
                        [
                            x[(c * rest + t) * upper : (c * rest + t + 1) * upper, h * lows : (h + 1) * lows]
                            for t in range(rest)
                        ],
                        axis=1,
                    )
                )
        return jnp.concatenate(pieces, axis=0)

    for step in range(sections):
        exchange(step)
        rnd, section = step // 4, step % 4
        recv = recvs[step]
        low = complex_matrix(gr_ref[rnd, section, 0], gi_ref[rnd, section, 0])
        mid = complex_matrix(
            jnp.concatenate([gr_ref[rnd, section, 1, pl.ds(t, upper, stride=rest), :] for t in range(rest)], axis=0),
            jnp.concatenate([gi_ref[rnd, section, 1, pl.ds(t, upper, stride=rest), :] for t in range(rest)], axis=0),
        )
        top = complex_matrix(gr_ref[rnd, section, 2], gi_ref[rnd, section, 2])
        if section in (1, 2):
            tall = jnp.concatenate(
                [
                    jnp.concatenate([recv[c, :, h].reshape(order, -1) for h in range(high)], axis=1)
                    for c in range(2)
                ],
                axis=0,
            )
        else:
            wide = jnp.concatenate([recv[c].reshape(high * order, lows) for c in range(2)], axis=1)
        if section == 2:
            wide = dot(low, tall, ((1,), (0,))).T
        elif section != 1:
            wide = dot(wide, low, ((1,), (1,)))
        if section != 1:
            tall = jnp.concatenate(
                [
                    jnp.concatenate(
                        [wide[h * order : (h + 1) * order, c * lows : (c + 1) * lows] for h in range(high)], axis=1
                    )
                    for c in range(2)
                ],
                axis=0,
            )
        out = dot(top, tops(dot(mid, tall, ((1,), (0,)))), ((1,), (0,)))
        for c in range(2):
            for h in range(high):
                for t in range(rest):
                    first = (c * high + h) * upper
                    part = out[first : first + upper, t * lows : (t + 1) * lows]
                    if section == 1:
                        x_ref[c, h, pl.ds(t, upper, stride=rest), :] = part
                    elif step == sections - 1:
                        (or_ref, oi_ref)[c][h, pl.ds(t, upper, stride=rest), :] = part
                    elif section == 0:
                        count = upper // nnear
                        for b in range(nnear):
                            sends[step][c, b, h, pl.ds(t, count, stride=rest), :] = part[
                                b * count : (b + 1) * count
                            ]
                    else:
                        n = nnear if section == 2 else nfar
                        count = high * upper // n
                        for i in range(n // high):
                            sends[step][c, h * (n // high) + i, pl.ds(t, count, stride=rest), :] = part[
                                i * count : (i + 1) * count
                            ]
        if section == 1:
            wide = jnp.concatenate([x_ref[c].reshape(high * order, lows) for c in range(2)], axis=1)
            turned = dot(low, wide, ((1,), (1,)))
            count = lows // nnear
            for c in range(2):
                for h in range(high):
                    for b in range(nnear):
                        first = c * lows + b * count
                        sends[step][c, b, h] = turned[first : first + count, h * order : (h + 1) * order]
    for copy in pending:
        copy.wait_send()


def one_kernel(nfar, nnear, state_real, state_imag, gate_real, gate_imag):
    shape = state_real.shape
    high, order, lows = shape[2:]
    rounds = gate_real.shape[0]
    sections = 4 * rounds
    kinds = (
        (2, nfar, high * order // nfar, lows),
        (2, nnear, high, order // nnear, lows),
        (2, nnear, high, lows // nnear, order),
        (2, nnear, high * order // nnear, lows),
    )
    buffers = [pltpu.VMEM(kinds[step % 4], jnp.float32) for step in range(sections)]
    most = max(nfar, nnear)
    vmem = pl.BlockSpec(memory_space=pltpu.VMEM)
    anywhere = pl.BlockSpec(memory_space=pl.ANY)
    result = jax.ShapeDtypeStruct((high, order, lows), jnp.float32)
    real, imag = pl.pallas_call(
        functools.partial(kernel, (nfar, nnear, rounds, high, order, lows)),
        out_shape=(result, result),
        in_specs=[vmem, vmem, anywhere, anywhere],
        out_specs=(vmem, vmem),
        scratch_shapes=buffers[1:]
        + buffers
        + [
            pltpu.VMEM(gate_real.shape, jnp.float32),
            pltpu.VMEM(gate_imag.shape, jnp.float32),
            pltpu.VMEM((2, high, order, lows), jnp.float32),
            pltpu.SemaphoreType.DMA((sections, 2, most)),
            pltpu.SemaphoreType.DMA((sections, 2, most)),
            pltpu.SemaphoreType.DMA((sections, 2)),
            pltpu.SemaphoreType.DMA((2,)),
        ],
        compiler_params=pltpu.CompilerParams(collective_id=0, has_side_effects=True),
    )(
        state_real.reshape(kinds[0][1:]),
        state_imag.reshape(kinds[0][1:]),
        gate_real,
        gate_imag,
    )
    return real.reshape(shape), imag.reshape(shape)


def solution(mesh):
    nfar, nnear = mesh.shape["far"], mesh.shape["near"]

    def body(state_real, state_imag, gate_real, gate_imag):
        high, order, lows = state_real.shape[2:]
        tiles = (high * order // nfar, order // high // nnear, lows // nnear, high * order // nnear)
        if any(rows < 8 or rows % 8 for rows in tiles):
            return on_device(state_real, state_imag, gate_real, gate_imag)
        return one_kernel(nfar, nnear, state_real, state_imag, gate_real, gate_imag)

    return jax.shard_map(
        body,
        mesh=mesh,
        in_specs=(P("far", "near", None, None, None), P("far", "near", None, None, None), P(), P()),
        out_specs=(P("far", "near", None, None, None), P("far", "near", None, None, None)),
        check_vma=False,
    )
```

```python
import functools

import jax
import jax.numpy as jnp
from jax import lax
from jax.experimental import pallas as pl
from jax.experimental.pallas import tpu as pltpu
from jax.sharding import PartitionSpec as P


def gate_low(x, g):
    return jnp.einsum(
        "...l,jl->...j", x, g, precision=lax.Precision.HIGHEST, preferred_element_type=jnp.float32
    )


def gate_mid(x, g):
    return jnp.einsum(
        "...ml,jm->...jl", x, g, precision=lax.Precision.HIGHEST, preferred_element_type=jnp.float32
    )


def gate_top(x, g):
    high, width, lows = (x.shape[-3], x.shape[-2], x.shape[-1])
    upper = g.shape[0] // high
    lead = x.shape[:-3]
    viewed = x.reshape(lead + (high, upper, width // upper, lows))
    matrix = g.reshape((g.shape[0], high, upper))
    out = jnp.einsum(
        "...hkrl,jhk->...jrl",
        viewed,
        matrix,
        precision=lax.Precision.HIGHEST,
        preferred_element_type=jnp.float32,
    )
    return out.reshape(lead + (high, width, lows))


def complex_gate(form, real, imag, greal, gimag):
    new_real = form(real, greal) - form(imag, gimag)
    new_imag = form(imag, greal) + form(real, gimag)
    return (new_real, new_imag)


def merged_rows(x):
    return x.reshape((1, 1, x.shape[2] * x.shape[3], x.shape[4]))


def on_device(state_real, state_imag, gate_real, gate_imag):
    real, imag = (state_real, state_imag)
    forms = (gate_low, gate_mid, gate_top)
    shape = state_real.shape
    for rnd in range(gate_real.shape[0]):
        for section in range(4):
            if section == 2:
                order = [1, 0, 2]
            else:
                order = [0, 1, 2]
            early = []
            later = order[len(early) :]
            pair = (real, imag)
            if section == 0:
                moved = (
                    lax.all_to_all(
                        merged_rows(pair[0]), "far", split_axis=2, concat_axis=2, tiled=True
                    ),
                    lax.all_to_all(
                        merged_rows(pair[1]), "far", split_axis=2, concat_axis=2, tiled=True
                    ),
                )
                pair = (moved[0].reshape(shape), moved[1].reshape(shape))
            elif section == 1:
                pair = (
                    lax.all_to_all(pair[0], "near", split_axis=3, concat_axis=3, tiled=True),
                    lax.all_to_all(pair[1], "near", split_axis=3, concat_axis=3, tiled=True),
                )
            elif section == 2:
                pair = (
                    lax.all_to_all(pair[0], "near", split_axis=4, concat_axis=4, tiled=True),
                    lax.all_to_all(pair[1], "near", split_axis=4, concat_axis=4, tiled=True),
                )
            else:
                moved = (
                    lax.all_to_all(
                        merged_rows(pair[0]), "near", split_axis=2, concat_axis=2, tiled=True
                    ),
                    lax.all_to_all(
                        merged_rows(pair[1]), "near", split_axis=2, concat_axis=2, tiled=True
                    ),
                )
                pair = (moved[0].reshape(shape), moved[1].reshape(shape))
            for which in later:
                pair = complex_gate(
                    forms[which],
                    pair[0],
                    pair[1],
                    gate_real[rnd, section, which],
                    gate_imag[rnd, section, which],
                )
            real, imag = pair
    return (real, imag)


def parts(x):
    first = x.astype(jnp.bfloat16)
    return first, (x - first.astype(jnp.float32)).astype(jnp.bfloat16)


def dot(a, b, dims):
    def product(x, y):
        return lax.dot_general(x, y, (dims, ((), ())), preferred_element_type=jnp.float32)

    return product(a[0], b[0]) + (product(a[0], b[1]) + product(a[1], b[0]))


def complex_matrix(greal, gimag):
    return jnp.concatenate(
        [jnp.concatenate([greal, -gimag], axis=1), jnp.concatenate([gimag, greal], axis=1)], axis=0
    )


def kernel(sizes, sr_ref, si_ref, gr_hbm, gi_hbm, or_ref, oi_ref, *scratch):
    nfar, nnear, rounds, high, order, lows = sizes
    sections = 4 * rounds
    sends, recvs = scratch[: sections - 1], scratch[sections - 1 : 2 * sections - 1]
    gr_ref, gi_ref, w_ref, x_ref, send_sem, recv_sem, own_sem, gate_sem = scratch[2 * sections - 1 :]
    far, near = lax.axis_index("far"), lax.axis_index("near")
    upper = order // high
    rest = order // upper

    loads = [
        pltpu.make_async_copy(gr_hbm, gr_ref, gate_sem.at[0]),
        pltpu.make_async_copy(gi_hbm, gi_ref, gate_sem.at[1]),
    ]
    for load in loads:
        load.start()
    barrier = pltpu.get_barrier_semaphore()
    for k in range(1, nfar):
        pl.semaphore_signal(
            barrier, inc=1, device_id=(lax.rem(far + k, nfar), near), device_id_type=pl.DeviceIdType.MESH
        )
    for k in range(1, nnear):
        pl.semaphore_signal(
            barrier, inc=1, device_id=(far, lax.rem(near + k, nnear)), device_id_type=pl.DeviceIdType.MESH
        )
    pl.semaphore_wait(barrier, nfar - 1 + nnear - 1)

    pending = []

    def launch(step, c):
        n, me = (nfar, far) if step % 4 == 0 else (nnear, near)
        source = (sr_ref, si_ref)[c] if step == 0 else sends[step - 1].at[c]
        recv = recvs[step].at[c]
        copies = []
        for k in range(1, n):
            to = lax.rem(me + k, n)
            copy = pltpu.make_async_remote_copy(
                src_ref=source.at[to],
                dst_ref=recv.at[me],
                send_sem=send_sem.at[step, c, k],
                recv_sem=recv_sem.at[step, c, k],
                device_id=(to, near) if step % 4 == 0 else (far, to),
                device_id_type=pl.DeviceIdType.MESH,
            )
            copy.start()
            pending.append(copy)
        own = pltpu.make_async_copy(source.at[me], recv.at[me], own_sem.at[step, c])
        own.start()

    def arrive(step, c):
        n, me = (nfar, far) if step % 4 == 0 else (nnear, near)
        recv = recvs[step].at[c]
        pltpu.make_async_copy(recv.at[me], recv.at[me], own_sem.at[step, c]).wait()
        for k in range(1, n):
            origin = lax.rem(me + n - k, n)
            pltpu.make_async_remote_copy(
                src_ref=recv.at[origin],
                dst_ref=recv.at[origin],
                send_sem=send_sem.at[step, c, k],
                recv_sem=recv_sem.at[step, c, k],
                device_id=(origin, near) if step % 4 == 0 else (far, origin),
                device_id_type=pl.DeviceIdType.MESH,
            ).wait_recv()

    def put(which, matrix):
        w_ref[which, 0], w_ref[which, 1] = parts(matrix)

    def get(which, rows, columns):
        return w_ref[which, 0, rows, columns], w_ref[which, 1, rows, columns]

    every = slice(None)

    def half(c):
        return slice(c * order, (c + 1) * order)

    def tops(x):
        pieces = []
        for c in range(2):
            for h in range(high):
                pieces.append(
                    jnp.concatenate(
                        [
                            x[(c * rest + t) * upper : (c * rest + t + 1) * upper, h * lows : (h + 1) * lows]
                            for t in range(rest)
                        ],
                        axis=1,
                    )
                )
        return jnp.concatenate(pieces, axis=0)

    for c in range(2):
        launch(0, c)
    for load in loads:
        load.wait()
    for step in range(sections):
        rnd, section = step // 4, step % 4
        recv = recvs[step]
        low = complex_matrix(gr_ref[rnd, section, 0], gi_ref[rnd, section, 0])
        put(0, low.T if section in (0, 3) else low)
        put(
            1,
            complex_matrix(
                jnp.concatenate(
                    [gr_ref[rnd, section, 1, pl.ds(t, upper, stride=rest), :] for t in range(rest)], axis=0
                ),
                jnp.concatenate(
                    [gi_ref[rnd, section, 1, pl.ds(t, upper, stride=rest), :] for t in range(rest)], axis=0
                ),
            ),
        )
        put(2, complex_matrix(gr_ref[rnd, section, 2], gi_ref[rnd, section, 2]))
        begun = []
        for c in range(2):
            arrive(step, c)
            if section in (1, 2):
                tall = jnp.concatenate([recv[c, :, h].reshape(order, -1) for h in range(high)], axis=1)
                begun.append(dot(get(2 - section, every, half(c)), parts(tall), ((1,), (0,))))
            else:
                wide = recv[c].reshape(high * order, lows)
                begun.append(dot(parts(wide), get(0, half(c), every), ((1,), (0,))))
        state = begun[0] + begun[1]
        if section != 1:
            wide = state.T if section == 2 else state
            tall = jnp.concatenate(
                [
                    jnp.concatenate(
                        [wide[h * order : (h + 1) * order, c * lows : (c + 1) * lows] for h in range(high)], axis=1
                    )
                    for c in range(2)
                ],
                axis=0,
            )
            state = dot(get(1, every, every), parts(tall), ((1,), (0,)))
        ready = parts(tops(state))
        for c in range(2):
            out = dot(get(2, half(c), every), ready, ((1,), (0,)))
            for h in range(high):
                for t in range(rest):
                    part = out[h * upper : (h + 1) * upper, t * lows : (t + 1) * lows]
                    if section == 1:
                        x_ref[c, h, pl.ds(t, upper, stride=rest), :] = part
                    elif step == sections - 1:
                        (or_ref, oi_ref)[c][h, pl.ds(t, upper, stride=rest), :] = part
                    elif section == 0:
                        count = upper // nnear
                        for b in range(nnear):
                            sends[step][c, b, h, pl.ds(t, count, stride=rest), :] = part[
                                b * count : (b + 1) * count
                            ]
                    else:
                        n = nnear if section == 2 else nfar
                        count = high * upper // n
                        for i in range(n // high):
                            sends[step][c, h * (n // high) + i, pl.ds(t, count, stride=rest), :] = part[
                                i * count : (i + 1) * count
                            ]
            if section != 1 and step < sections - 1:
                launch(step + 1, c)
        if section == 1:
            wide = parts(jnp.concatenate([x_ref[c].reshape(high * order, lows) for c in range(2)], axis=1))
            count = lows // nnear
            for c in range(2):
                turned = dot(get(0, half(c), every), wide, ((1,), (1,)))
                for h in range(high):
                    for b in range(nnear):
                        sends[step][c, b, h] = turned[b * count : (b + 1) * count, h * order : (h + 1) * order]
                launch(step + 1, c)
    for copy in pending:
        copy.wait_send()


def one_kernel(nfar, nnear, state_real, state_imag, gate_real, gate_imag):
    shape = state_real.shape
    high, order, lows = shape[2:]
    rounds = gate_real.shape[0]
    sections = 4 * rounds
    kinds = (
        (2, nfar, high * order // nfar, lows),
        (2, nnear, high, order // nnear, lows),
        (2, nnear, high, lows // nnear, order),
        (2, nnear, high * order // nnear, lows),
    )
    buffers = [pltpu.VMEM(kinds[step % 4], jnp.float32) for step in range(sections)]
    most = max(nfar, nnear)
    vmem = pl.BlockSpec(memory_space=pltpu.VMEM)
    anywhere = pl.BlockSpec(memory_space=pl.ANY)
    result = jax.ShapeDtypeStruct((high, order, lows), jnp.float32)
    real, imag = pl.pallas_call(
        functools.partial(kernel, (nfar, nnear, rounds, high, order, lows)),
        out_shape=(result, result),
        in_specs=[vmem, vmem, anywhere, anywhere],
        out_specs=(vmem, vmem),
        scratch_shapes=buffers[1:]
        + buffers
        + [
            pltpu.VMEM(gate_real.shape, jnp.float32),
            pltpu.VMEM(gate_imag.shape, jnp.float32),
            pltpu.VMEM((3, 2, 2 * order, 2 * order), jnp.bfloat16),
            pltpu.VMEM((2, high, order, lows), jnp.float32),
            pltpu.SemaphoreType.DMA((sections, 2, most)),
            pltpu.SemaphoreType.DMA((sections, 2, most)),
            pltpu.SemaphoreType.DMA((sections, 2)),
            pltpu.SemaphoreType.DMA((2,)),
        ],
        compiler_params=pltpu.CompilerParams(collective_id=0, has_side_effects=True),
    )(
        state_real.reshape(kinds[0][1:]),
        state_imag.reshape(kinds[0][1:]),
        gate_real,
        gate_imag,
    )
    return real.reshape(shape), imag.reshape(shape)


def solution(mesh):
    nfar, nnear = mesh.shape["far"], mesh.shape["near"]

    def body(state_real, state_imag, gate_real, gate_imag):
        high, order, lows = state_real.shape[2:]
        tiles = (high * order // nfar, order // high // nnear, lows // nnear, high * order // nnear)
        if any(rows < 8 or rows % 8 for rows in tiles):
            return on_device(state_real, state_imag, gate_real, gate_imag)
        return one_kernel(nfar, nnear, state_real, state_imag, gate_real, gate_imag)

    return jax.shard_map(
        body,
        mesh=mesh,
        in_specs=(P("far", "near", None, None, None), P("far", "near", None, None, None), P(), P()),
        out_specs=(P("far", "near", None, None, None), P("far", "near", None, None, None)),
        check_vma=False,
    )
```

```python
import functools

import jax
import jax.numpy as jnp
from jax import lax
from jax.experimental import pallas as pl
from jax.experimental.pallas import tpu as pltpu
from jax.sharding import PartitionSpec as P


def gate_low(x, g):
    return jnp.einsum(
        "...l,jl->...j", x, g, precision=lax.Precision.HIGHEST, preferred_element_type=jnp.float32
    )


def gate_mid(x, g):
    return jnp.einsum(
        "...ml,jm->...jl", x, g, precision=lax.Precision.HIGHEST, preferred_element_type=jnp.float32
    )


def gate_top(x, g):
    high, width, lows = (x.shape[-3], x.shape[-2], x.shape[-1])
    upper = g.shape[0] // high
    lead = x.shape[:-3]
    viewed = x.reshape(lead + (high, upper, width // upper, lows))
    matrix = g.reshape((g.shape[0], high, upper))
    out = jnp.einsum(
        "...hkrl,jhk->...jrl",
        viewed,
        matrix,
        precision=lax.Precision.HIGHEST,
        preferred_element_type=jnp.float32,
    )
    return out.reshape(lead + (high, width, lows))


def complex_gate(form, real, imag, greal, gimag):
    new_real = form(real, greal) - form(imag, gimag)
    new_imag = form(imag, greal) + form(real, gimag)
    return (new_real, new_imag)


def merged_rows(x):
    return x.reshape((1, 1, x.shape[2] * x.shape[3], x.shape[4]))


def on_device(state_real, state_imag, gate_real, gate_imag):
    real, imag = (state_real, state_imag)
    forms = (gate_low, gate_mid, gate_top)
    shape = state_real.shape
    for rnd in range(gate_real.shape[0]):
        for section in range(4):
            if section == 2:
                order = [1, 0, 2]
            else:
                order = [0, 1, 2]
            early = []
            later = order[len(early) :]
            pair = (real, imag)
            if section == 0:
                moved = (
                    lax.all_to_all(
                        merged_rows(pair[0]), "far", split_axis=2, concat_axis=2, tiled=True
                    ),
                    lax.all_to_all(
                        merged_rows(pair[1]), "far", split_axis=2, concat_axis=2, tiled=True
                    ),
                )
                pair = (moved[0].reshape(shape), moved[1].reshape(shape))
            elif section == 1:
                pair = (
                    lax.all_to_all(pair[0], "near", split_axis=3, concat_axis=3, tiled=True),
                    lax.all_to_all(pair[1], "near", split_axis=3, concat_axis=3, tiled=True),
                )
            elif section == 2:
                pair = (
                    lax.all_to_all(pair[0], "near", split_axis=4, concat_axis=4, tiled=True),
                    lax.all_to_all(pair[1], "near", split_axis=4, concat_axis=4, tiled=True),
                )
            else:
                moved = (
                    lax.all_to_all(
                        merged_rows(pair[0]), "near", split_axis=2, concat_axis=2, tiled=True
                    ),
                    lax.all_to_all(
                        merged_rows(pair[1]), "near", split_axis=2, concat_axis=2, tiled=True
                    ),
                )
                pair = (moved[0].reshape(shape), moved[1].reshape(shape))
            for which in later:
                pair = complex_gate(
                    forms[which],
                    pair[0],
                    pair[1],
                    gate_real[rnd, section, which],
                    gate_imag[rnd, section, which],
                )
            real, imag = pair
    return (real, imag)


def parts(x):
    first = x.astype(jnp.bfloat16)
    return first, (x - first.astype(jnp.float32)).astype(jnp.bfloat16)


def dot(a, b, dims):
    def product(x, y):
        return lax.dot_general(x, y, (dims, ((), ())), preferred_element_type=jnp.float32)

    return product(a[0], b[0]) + (product(a[0], b[1]) + product(a[1], b[0]))


def complex_matrix(greal, gimag):
    return jnp.concatenate(
        [jnp.concatenate([greal, -gimag], axis=1), jnp.concatenate([gimag, greal], axis=1)], axis=0
    )


def kernel(sizes, sr_ref, si_ref, gr_hbm, gi_hbm, or_ref, oi_ref, *scratch):
    nfar, nnear, rounds, high, order, lows = sizes
    sections = 4 * rounds
    sends, recvs = scratch[: sections - 1], scratch[sections - 1 : 2 * sections - 1]
    gr_ref, gi_ref, w_ref, x_ref, send_sem, recv_sem, own_sem, gate_sem = scratch[2 * sections - 1 :]
    far, near = lax.axis_index("far"), lax.axis_index("near")
    upper = order // high
    rest = order // upper

    loads = [
        pltpu.make_async_copy(gr_hbm, gr_ref, gate_sem.at[0]),
        pltpu.make_async_copy(gi_hbm, gi_ref, gate_sem.at[1]),
    ]
    for load in loads:
        load.start()
    barrier = pltpu.get_barrier_semaphore()
    for k in range(1, nfar):
        pl.semaphore_signal(
            barrier, inc=1, device_id=(lax.rem(far + k, nfar), near), device_id_type=pl.DeviceIdType.MESH
        )
    for k in range(1, nnear):
        pl.semaphore_signal(
            barrier, inc=1, device_id=(far, lax.rem(near + k, nnear)), device_id_type=pl.DeviceIdType.MESH
        )
    pl.semaphore_wait(barrier, nfar - 1 + nnear - 1)

    pending = []

    def launch(step, c):
        n, me = (nfar, far) if step % 4 == 0 else (nnear, near)
        source = (sr_ref, si_ref)[c] if step == 0 else sends[step - 1].at[c]
        recv = recvs[step].at[c]
        copies = []
        for k in range(1, n):
            to = lax.rem(me + k, n)
            copy = pltpu.make_async_remote_copy(
                src_ref=source.at[to],
                dst_ref=recv.at[me],
                send_sem=send_sem.at[step, c, k],
                recv_sem=recv_sem.at[step, c, k],
                device_id=(to, near) if step % 4 == 0 else (far, to),
                device_id_type=pl.DeviceIdType.MESH,
            )
            copy.start()
            pending.append(copy)
        own = pltpu.make_async_copy(source.at[me], recv.at[me], own_sem.at[step, c])
        own.start()

    def arrive(step, c):
        n, me = (nfar, far) if step % 4 == 0 else (nnear, near)
        recv = recvs[step].at[c]
        pltpu.make_async_copy(recv.at[me], recv.at[me], own_sem.at[step, c]).wait()
        for k in range(1, n):
            origin = lax.rem(me + n - k, n)
            pltpu.make_async_remote_copy(
                src_ref=recv.at[origin],
                dst_ref=recv.at[origin],
                send_sem=send_sem.at[step, c, k],
                recv_sem=recv_sem.at[step, c, k],
                device_id=(origin, near) if step % 4 == 0 else (far, origin),
                device_id_type=pl.DeviceIdType.MESH,
            ).wait_recv()

    def put(which, matrix):
        w_ref[which, 0], w_ref[which, 1] = parts(matrix)

    def get(which, rows, columns):
        return w_ref[which, 0, rows, columns], w_ref[which, 1, rows, columns]

    every = slice(None)

    def half(c):
        return slice(c * order, (c + 1) * order)

    def tops(x):
        pieces = []
        for c in range(2):
            for h in range(high):
                pieces.append(
                    jnp.concatenate(
                        [
                            x[(c * rest + t) * upper : (c * rest + t + 1) * upper, h * lows : (h + 1) * lows]
                            for t in range(rest)
                        ],
                        axis=1,
                    )
                )
        return jnp.concatenate(pieces, axis=0)

    for c in range(2):
        launch(0, c)
    for load in loads:
        load.wait()
    for step in range(sections):
        rnd, section = step // 4, step % 4
        recv = recvs[step]
        low = complex_matrix(gr_ref[rnd, section, 0], gi_ref[rnd, section, 0])
        put(0, low.T if section in (0, 3) else low)
        put(
            1,
            complex_matrix(
                jnp.concatenate(
                    [gr_ref[rnd, section, 1, pl.ds(t, upper, stride=rest), :] for t in range(rest)], axis=0
                ),
                jnp.concatenate(
                    [gi_ref[rnd, section, 1, pl.ds(t, upper, stride=rest), :] for t in range(rest)], axis=0
                ),
            ),
        )
        put(2, complex_matrix(gr_ref[rnd, section, 2], gi_ref[rnd, section, 2]))
        begun = []
        for c in range(2):
            arrive(step, c)
            if section in (1, 2):
                tall = jnp.concatenate([recv[c, :, h].reshape(order, -1) for h in range(high)], axis=1)
                begun.append(dot(get(2 - section, every, half(c)), parts(tall), ((1,), (0,))))
            else:
                wide = recv[c].reshape(high * order, lows)
                begun.append(dot(parts(wide), get(0, half(c), every), ((1,), (0,))))
        state = begun[0] + begun[1]
        if section != 1:
            wide = state.T if section == 2 else state
            tall = jnp.concatenate(
                [
                    jnp.concatenate(
                        [wide[h * order : (h + 1) * order, c * lows : (c + 1) * lows] for h in range(high)], axis=1
                    )
                    for c in range(2)
                ],
                axis=0,
            )
            state = dot(get(1, every, every), parts(tall), ((1,), (0,)))
        ready = parts(tops(state))
        for c in range(2):
            out = dot(get(2, half(c), every), ready, ((1,), (0,)))
            for h in range(high):
                for t in range(rest):
                    part = out[h * upper : (h + 1) * upper, t * lows : (t + 1) * lows]
                    if section == 1:
                        x_ref[c, h, pl.ds(t, upper, stride=rest), :] = part
                    elif step == sections - 1:
                        (or_ref, oi_ref)[c][h, pl.ds(t, upper, stride=rest), :] = part
                    elif section == 0:
                        count = upper // nnear
                        for b in range(nnear):
                            sends[step][c, b, h, pl.ds(t, count, stride=rest), :] = part[
                                b * count : (b + 1) * count
                            ]
                    else:
                        n = nnear if section == 2 else nfar
                        count = high * upper // n
                        for i in range(n // high):
                            sends[step][c, h * (n // high) + i, pl.ds(t, count, stride=rest), :] = part[
                                i * count : (i + 1) * count
                            ]
            if section != 1 and step < sections - 1:
                launch(step + 1, c)
        if section == 1:
            wide = parts(jnp.concatenate([x_ref[c].reshape(high * order, lows) for c in range(2)], axis=1))
            count = lows // nnear
            for c in range(2):
                turned = dot(get(0, half(c), every), wide, ((1,), (1,)))
                for h in range(high):
                    for b in range(nnear):
                        sends[step][c, b, h] = turned[b * count : (b + 1) * count, h * order : (h + 1) * order]
                launch(step + 1, c)
    for copy in pending:
        copy.wait_send()


def one_kernel(nfar, nnear, state_real, state_imag, gate_real, gate_imag):
    shape = state_real.shape
    high, order, lows = shape[2:]
    rounds = gate_real.shape[0]
    sections = 4 * rounds
    kinds = (
        (2, nfar, high * order // nfar, lows),
        (2, nnear, high, order // nnear, lows),
        (2, nnear, high, lows // nnear, order),
        (2, nnear, high * order // nnear, lows),
    )
    buffers = [pltpu.VMEM(kinds[step % 4], jnp.float32) for step in range(sections)]
    most = max(nfar, nnear)
    vmem = pl.BlockSpec(memory_space=pltpu.VMEM)
    anywhere = pl.BlockSpec(memory_space=pl.ANY)
    result = pltpu.VMEM((high, order, lows), jnp.float32)
    real, imag = pl.pallas_call(
        functools.partial(kernel, (nfar, nnear, rounds, high, order, lows)),
        out_shape=(result, result),
        in_specs=[vmem, vmem, anywhere, anywhere],
        out_specs=(vmem, vmem),
        scratch_shapes=buffers[1:]
        + buffers
        + [
            pltpu.VMEM(gate_real.shape, jnp.float32),
            pltpu.VMEM(gate_imag.shape, jnp.float32),
            pltpu.VMEM((3, 2, 2 * order, 2 * order), jnp.bfloat16),
            pltpu.VMEM((2, high, order, lows), jnp.float32),
            pltpu.SemaphoreType.DMA((sections, 2, most)),
            pltpu.SemaphoreType.DMA((sections, 2, most)),
            pltpu.SemaphoreType.DMA((sections, 2)),
            pltpu.SemaphoreType.DMA((2,)),
        ],
        compiler_params=pltpu.CompilerParams(collective_id=0, has_side_effects=True),
    )(
        state_real.reshape(kinds[0][1:]),
        state_imag.reshape(kinds[0][1:]),
        gate_real,
        gate_imag,
    )
    return real.reshape(shape), imag.reshape(shape)


def solution(mesh):
    nfar, nnear = mesh.shape["far"], mesh.shape["near"]

    def body(state_real, state_imag, gate_real, gate_imag):
        high, order, lows = state_real.shape[2:]
        tiles = (high * order // nfar, order // high // nnear, lows // nnear, high * order // nnear)
        if any(rows < 8 or rows % 8 for rows in tiles):
            return on_device(state_real, state_imag, gate_real, gate_imag)
        return one_kernel(nfar, nnear, state_real, state_imag, gate_real, gate_imag)

    return jax.shard_map(
        body,
        mesh=mesh,
        in_specs=(P("far", "near", None, None, None), P("far", "near", None, None, None), P(), P()),
        out_specs=(P("far", "near", None, None, None), P("far", "near", None, None, None)),
        check_vma=False,
    )
```
